32 devices in a mesh: dp: 2 (over x), tp: 16 (over y, z, core).
Axes of the slice: x: 2, y: 2, z: 4, core: 2. Of those that a mesh axis runs over, the one named last changes fastest.
Arguments:
- x: bfloat16 [8192, 4096], P(('dp', 'tp')), parts along dimension 0
- w_gate: bfloat16 [4096, 12288], P(None, 'tp')
- w_up: bfloat16 [4096, 12288], P(None, 'tp')
- w_down: bfloat16 [12288, 4096], P('tp')
Outputs:
- output: bfloat16 [8192, 4096], P(('dp', 'tp')), parts along dimension 0
There are 2 independent parts. The reference program is written for one: setup_inputs(seed, part) draws one part's arguments, and reference() takes and returns one part's arrays. A program takes and returns all parts, laid end to end along the dimension named above; an argument that names none is the same for every part.
All inputs are finite; a program needn't handle non-finite values.
Results may differ from the reference program's by a relative error of at most 0.016.
Values are sent between devices in bfloat16 or wider.
A program may use at most 2 GiB of HBM per device.

```python
import jax
import jax.numpy as jnp

ROWS = 4096
D = 4096
FF = 12288


def setup_inputs(seed: int = 0, part: int = 0) -> dict:
    kx, kg, ku, kd = jax.random.split(jax.random.key(seed), 4)
    drawn = {
        "x": jax.random.normal(jax.random.fold_in(kx, part), (ROWS, D), jnp.float32),
        "w_gate": jax.random.normal(kg, (D, FF), jnp.float32) * D**-0.5,
        "w_up": jax.random.normal(ku, (D, FF), jnp.float32) * D**-0.5,
        "w_down": jax.random.normal(kd, (FF, D), jnp.float32) * FF**-0.5,
    }
    return {k: v.astype(jnp.bfloat16) for k, v in drawn.items()}


def reference(x, w_gate, w_up, w_down):
    gate = jnp.dot(x, w_gate, preferred_element_type=jnp.float32)
    up = jnp.dot(x, w_up, preferred_element_type=jnp.float32)
    hidden = (jax.nn.silu(gate) * up).astype(jnp.bfloat16)
    return jnp.dot(hidden, w_down, preferred_element_type=jnp.float32).astype(jnp.bfloat16)
```

```python
import functools

import jax
import jax.numpy as jnp
from jax import lax
from jax.experimental import pallas as pl
from jax.experimental.pallas import tpu as pltpu
from jax.sharding import PartitionSpec as P

CHIPS = 8
SLOTS = 4
MESH = pl.DeviceIdType.MESH


def chip_at(place):
    return jnp.where(place < 4, place, 11 - place)


def kernel(x_ref, wg_ref, wu_ref, wd_ref, out_ref, sum_ref,
           wg, wu, wd, xb, acc, own, hid, term, stage, other, got,
           w_sem, own_sem, load_sem, out_sem,
           x_send, x_recv, d_send, d_recv, t_send, t_recv, s_send, s_recv):
    rows = xb.shape[2] // 2
    depth, cols = wg.shape
    wide = wd.shape[1]
    tile = 512
    last = CHIPS - 1

    dp = lax.axis_index("dp")
    tp = lax.axis_index("tp")
    core = lax.rem(tp, 2)
    chip = tp // 2
    place = jnp.where(chip < 4, chip, 11 - chip)
    right = (dp, chip_at(lax.rem(place + 1, CHIPS)) * 2 + core)
    left = (dp, chip_at(lax.rem(place + CHIPS - 1, CHIPS)) * 2 + core)
    mate = (dp, tp + 1 - 2 * core)
    onward = (right, left)

    loads = [
        pltpu.make_async_copy(src, dst, w_sem.at[n])
        for n, (src, dst) in enumerate(((wg_ref, wg), (wu_ref, wu), (wd_ref, wd)))
    ]
    mine = [
        pltpu.make_async_copy(
            x_ref.at[pl.ds(d * rows, rows)], xb.at[d, 0, pl.ds(0, rows)], own_sem.at[d]
        )
        for d in range(2)
    ]
    for copy in mine + loads:
        copy.start()

    barrier = pltpu.get_barrier_semaphore()
    for peer in (left, right, mate):
        pl.semaphore_signal(barrier, inc=1, device_id=peer, device_id_type=MESH)
    pl.semaphore_wait(barrier, 3)

    def remote(src, dst, send, recv, peer):
        return pltpu.make_async_remote_copy(
            src_ref=src, dst_ref=dst, send_sem=send, recv_sem=recv,
            device_id=peer, device_id_type=MESH,
        )

    def pass_on(d, k, src=None):
        if src is None:
            src = xb.at[d, lax.rem(k, SLOTS), pl.ds(0, rows)]
        return remote(
            src, xb.at[d, lax.rem(k + 1, SLOTS), pl.ds(0, rows)],
            x_send.at[d, k], x_recv.at[d, k + 1], onward[d],
        )

    def share(d, k, src=None):
        slot = lax.rem(k, SLOTS)
        if src is None:
            src = xb.at[d, slot, pl.ds(0, rows)]
        return remote(
            src, xb.at[d, slot, pl.ds(rows, rows)], d_send.at[d, k], d_recv.at[d, k], mate
        )

    def give(d, k):
        return remote(
            term.at[d], other.at[d, lax.rem(k, 2)], t_send.at[d, k], t_recv.at[d, k], mate
        )

    def advance(d, k):
        return remote(
            stage.at[d, lax.rem(k, 2)], sum_ref.at[d, k + 1],
            s_send.at[d, k], s_recv.at[d, k + 1], onward[d],
        )

    def fetch(d, k):
        return pltpu.make_async_copy(sum_ref.at[d, k], got.at[d], load_sem.at[d])

    for d in range(2):
        pass_on(d, 0, x_ref.at[pl.ds(d * rows, rows)]).start()
    for d in range(2):
        share(d, 0, x_ref.at[pl.ds(d * rows, rows)]).start()
    for copy in mine + loads:
        copy.wait()

    def terms(d, k):
        slot = lax.rem(k, SLOTS)
        share(d, k).wait_recv()
        for n in range(cols // 256):
            part = pl.ds(n * 256, 256)
            gate = jnp.dot(xb[d, slot], wg[:, part], preferred_element_type=jnp.float32)
            up = jnp.dot(xb[d, slot], wu[:, part], preferred_element_type=jnp.float32)
            hid[:, part] = (jax.nn.silu(gate) * up).astype(hid.dtype)

        @pl.when(k > 0)
        def _():
            give(d, k - 1).wait_send()

        for n in range(wide // tile):
            part = pl.ds(n * tile, tile)
            both = jnp.dot(hid[...], wd[:, part], preferred_element_type=jnp.float32)
            acc[d, :, part] = both[:rows]
            term[d, :, part] = both[rows:].astype(term.dtype)
        give(d, k).start()

    def add(d, k):
        give(d, k).wait_recv()

        @pl.when(k >= 2)
        def _():
            fetch(d, k).wait()
            for n in range(wide // tile):
                part = pl.ds(n * tile, tile)
                acc[d, :, part] += got[d, :, part].astype(jnp.float32)

        slot = lax.rem(k, 2)

        @pl.when(k == 0)
        def _():
            for n in range(wide // tile):
                part = pl.ds(n * tile, tile)
                own[d, :, part] = acc[d, :, part] + other[d, slot, :, part].astype(jnp.float32)

        @pl.when(k >= 3)
        def _():
            advance(d, k - 2).wait_send()

        @pl.when(k >= 1)
        def _():
            for n in range(wide // tile):
                part = pl.ds(n * tile, tile)
                stage[d, slot, :, part] = (
                    acc[d, :, part] + other[d, slot, :, part].astype(jnp.float32)
                ).astype(stage.dtype)
            advance(d, k).start()

    @pl.loop(0, CHIPS)
    def _(k):
        @pl.when(k >= 1)
        def _():
            for d in range(2):
                pass_on(d, k - 1).wait_recv()

                @pl.when(k < last)
                def _():
                    pass_on(d, k).start()

                share(d, k).start()

        for d in range(2):
            terms(d, k)

        @pl.when(k >= 1)
        def _():
            for d in range(2):
                pass_on(d, k - 1).wait_send()
                share(d, k - 1).wait_send()

        @pl.when(k >= 2)
        def _():
            for d in range(2):
                advance(d, k - 1).wait_recv()
                fetch(d, k).start()

        for d in range(2):
            add(d, k)

    for d in range(2):
        advance(d, last).wait_recv()
        fetch(d, CHIPS).start()
    results = []
    for d in range(2):
        fetch(d, CHIPS).wait()
        advance(d, last - 1).wait_send()
        for n in range(wide // tile):
            part = pl.ds(n * tile, tile)
            stage[d, (last - 1) % 2, :, part] = (
                own[d, :, part] + got[d, :, part].astype(jnp.float32)
            ).astype(stage.dtype)
        copy = pltpu.make_async_copy(
            stage.at[d, (last - 1) % 2], out_ref.at[pl.ds(d * rows, rows)], out_sem.at[d]
        )
        copy.start()
        results.append(copy)
    for d in range(2):
        share(d, last).wait_send()
        give(d, last).wait_send()
        advance(d, last).wait_send()
        results[d].wait()


def solution(mesh):
    def step(x, w_gate, w_up, w_down):
        total, depth = x.shape
        rows = total // 2
        cols = w_gate.shape[1]
        wide = w_down.shape[1]
        dma = pltpu.SemaphoreType.DMA
        hops = (2, CHIPS + 1)
        b16, f32 = jnp.bfloat16, jnp.float32
        anywhere = pl.BlockSpec(memory_space=pl.ANY)
        out, _ = pl.pallas_call(
            kernel,
            name="ring",
            out_shape=(
                jax.ShapeDtypeStruct((total, wide), b16),
                jax.ShapeDtypeStruct((2, CHIPS + 1, rows, wide), b16),
            ),
            in_specs=[anywhere] * 4,
            out_specs=(anywhere, anywhere),
            scratch_shapes=[
                pltpu.VMEM((depth, cols), b16),
                pltpu.VMEM((depth, cols), b16),
                pltpu.VMEM((cols, wide), b16),
                pltpu.VMEM((2, SLOTS, 2 * rows, depth), b16),
                pltpu.VMEM((2, rows, wide), f32),
                pltpu.VMEM((2, rows, wide), f32),
                pltpu.VMEM((2 * rows, cols), b16),
                pltpu.VMEM((2, rows, wide), b16),
                pltpu.VMEM((2, 2, rows, wide), b16),
                pltpu.VMEM((2, 2, rows, wide), b16),
                pltpu.VMEM((2, rows, wide), b16),
                dma((3,)), dma((2,)), dma((2,)), dma((2,)),
                dma(hops), dma(hops), dma(hops), dma(hops),
                dma(hops), dma(hops), dma(hops), dma(hops),
            ],
            compiler_params=pltpu.CompilerParams(
                collective_id=0, has_side_effects=True, vmem_limit_bytes=67043328
            ),
            cost_estimate=pl.CostEstimate(
                flops=2 * 16 * total * depth * cols * 3,
                bytes_accessed=3 * depth * cols * 2 + 64 * total * depth * 2,
                transcendentals=16 * total * cols,
            ),
        )(x, w_gate, w_up, w_down)
        return out

    return jax.shard_map(
        step,
        mesh=mesh,
        in_specs=(P(("dp", "tp"), None), P(None, "tp"), P(None, "tp"), P("tp", None)),
        out_specs=P(("dp", "tp"), None),
        check_vma=False,
    )
```

```python
import functools

import jax
import jax.numpy as jnp
from jax import lax
from jax.experimental import pallas as pl
from jax.experimental.pallas import tpu as pltpu
from jax.sharding import PartitionSpec as P

PARTS = 4
STAGES = 8
MESH = pl.DeviceIdType.MESH
PASS = (
    (
        5, 28, 13, 20, 57, 140, 49, 33, 89, 169, 160, 97,
        209, 216, 193, 224, 184, 233, 80, 40, 144, 64, 176, 152,
        104, 241, 248, 200, 112, 120, 72, 128,
    ),
    (
        62, 51, 45, 39, 91, 5, 180, 65, 170, 160, 98, 140,
        17, 29, 211, 194, 150, 234, 158, 80, 220, 132, 75, 243,
        12, 250, 224, 202, 184, 122, 104, 112,
    ),
)
PASS_END = (
    (
        9, 11, 11, 13, 16, 16, 16, 16, 21, 21, 22, 23,
        26, 26, 26, 26, 27, 29, 29, 30, 30, 31, 32, 32,
        32, 32, 32, 32, 32, 32, 32, 32,
    ),
    (
        12, 16, 19, 24, 24, 25, 26, 27, 27, 29, 29, 29,
        29, 29, 29, 31, 31, 31, 31, 31, 32, 32, 32, 32,
        32, 32, 32, 32, 32, 32, 32, 32,
    ),
)
WORK = (
    (
        131, 355, 643, 387, 867, 675, 833, 899, 769, 929, 579, 327,
        737, 263, 423, 961, 231, 993, 455, 801, 487, 721, 545, 295,
        529, 199, 625, 52, 163, 80, 20, 116,
    ),
    (
        545, 833, 769, 961, 929, 395, 875, 363, 993, 649, 907, 18,
        585, 801, 335, 753, 706, 271, 530, 431, 610, 681, 156, 463,
        54, 495, 86, 303, 114, 252, 216, 188,
    ),
)


def kernel(x_ref, wg_ref, wu_ref, wd_ref, out_ref, sum_ref,
           wg, wu, wd, xb, acc, hid, term, other, got, stage,
           w_sem, own_sem, load_sem,
           x_send, x_recv, d_send, d_recv, t_send, t_recv, s_send, s_recv):
    chunks = 8 * PARTS
    rows = xb.shape[1] // 2
    depth, cols = wg.shape
    wide = wd.shape[1]
    tile = 512

    dp = lax.axis_index("dp")
    tp = lax.axis_index("tp")
    core = lax.rem(tp, 2)
    chip = tp // 2
    y = chip // 4
    z = lax.rem(chip, 4)
    flip = z // 2
    outer = (z == 0) | (z == 3)
    away = 2 - 4 * flip
    mate = (dp, tp + 1 - 2 * core)
    peers = ((dp, tp + 8 - 16 * y), (dp, tp - away), (dp, tp + away))

    def pick(table, i):
        value = jnp.where(outer, table[0][0], table[1][0])
        for n in range(1, len(table[0])):
            value = jnp.where(i == n, jnp.where(outer, table[0][n], table[1][n]), value)
        return value

    def slot_of(chunk):
        source = chunk // PARTS
        sy = lax.rem(source // 4 + y, 2)
        sz = lax.rem(source, 4)
        sz = sz + flip * (3 - 2 * sz)
        return (sy * 4 + sz) * PARTS + lax.rem(chunk, PARTS)

    def bit(mask, n):
        return lax.rem(mask // (1 << n), 2) == 1

    loads = [
        pltpu.make_async_copy(src, dst, w_sem.at[n])
        for n, (src, dst) in enumerate(((wg_ref, wg), (wu_ref, wu), (wd_ref, wd)))
    ]
    mine = [
        pltpu.make_async_copy(
            x_ref.at[pl.ds(q * rows, rows)],
            xb.at[chip * PARTS + q, pl.ds(0, rows)],
            own_sem.at[q],
        )
        for q in range(PARTS)
    ]
    for copy in mine + loads:
        copy.start()

    barrier = pltpu.get_barrier_semaphore()
    for peer in (mate, peers[0], peers[2]):
        pl.semaphore_signal(barrier, inc=1, device_id=peer, device_id_type=MESH)

    @pl.when(jnp.logical_not(outer))
    def _():
        pl.semaphore_signal(barrier, inc=1, device_id=peers[1], device_id_type=MESH)

    pl.semaphore_wait(barrier, jnp.where(outer, 3, 4))

    def remote(src, dst, send, recv, peer):
        return pltpu.make_async_remote_copy(
            src_ref=src, dst_ref=dst, send_sem=send, recv_sem=recv,
            device_id=peer, device_id_type=MESH,
        )

    def rows_to(link, slot, src=None):
        here = xb.at[slot, pl.ds(0, rows)]
        return remote(
            here if src is None else src, here,
            x_send.at[link, slot], x_recv.at[slot], peers[link],
        )

    def share(slot, src=None):
        return remote(
            xb.at[slot, pl.ds(0, rows)] if src is None else src,
            xb.at[slot, pl.ds(rows, rows)],
            d_send.at[slot], d_recv.at[slot], mate,
        )

    def give(i):
        n = lax.rem(i, 2)
        return remote(term.at[n], other.at[n], t_send.at[n], t_recv.at[n], mate)

    def landing(slot, link):
        return sum_ref.at[slot * 3 + link]

    def fetch(slot, link):
        return pltpu.make_async_copy(landing(slot, link), got.at[link], load_sem.at[link])

    def sum_to(i, slot, link):
        n = lax.rem(i, STAGES)
        there = 0 if link == 0 else 2 if link == 1 else jnp.where(outer, 1, 2)
        return remote(
            stage.at[n], landing(slot, there), s_send.at[n], s_recv.at[slot * 3 + there],
            peers[link],
        )

    def keep(i, slot):
        n = lax.rem(i, STAGES)
        q = lax.rem(slot, PARTS)
        return pltpu.make_async_copy(
            stage.at[n], out_ref.at[pl.ds(pl.multiple_of(q * rows, rows), rows)], s_send.at[n]
        )

    def sent(i):
        n = lax.rem(i, STAGES)
        pltpu.make_async_copy(stage.at[n], stage.at[n], s_send.at[n]).wait()

    def pass_on(j, own=False):
        code = pick(PASS, j)
        chunk = code // 8
        mask = lax.rem(code, 8)
        slot = slot_of(chunk)
        src = None
        if own:
            q = lax.rem(chunk, PARTS)
            src = x_ref.at[pl.ds(pl.multiple_of(q * rows, rows), rows)]
        else:
            rows_to(0, slot).wait_recv()
        for link in (2, 1, 0):

            @pl.when(bit(mask, link))
            def _():
                rows_to(link, slot, src).start()

        share(slot, src).start()

    for j in range(PARTS):
        pass_on(j, own=True)
    for copy in mine + loads:
        copy.wait()

    @pl.loop(0, chunks + 1)
    def _(i):
        begin = jnp.where(i == 0, PARTS, pick(PASS_END, jnp.maximum(i - 1, 0)))
        end = pick(PASS_END, jnp.minimum(i, chunks - 1))

        def passing(j, carry):
            pass_on(j)
            return carry

        lax.fori_loop(begin, end, passing, 0)

        before = pick(WORK, jnp.maximum(i - 1, 0))
        slot_before = slot_of(before // 32)
        arriving = lax.rem(before // 4, 8)
        leaving = lax.rem(before, 4)

        @pl.when(i >= 1)
        def _():
            for link in range(3):

                @pl.when(bit(arriving, link))
                def _():
                    remote(
                        landing(slot_before, link), landing(slot_before, link),
                        s_send.at[0], s_recv.at[slot_before * 3 + link], mate,
                    ).wait_recv()
                    fetch(slot_before, link).start()

        @pl.when(i < chunks)
        def _():
            slot = slot_of(pick(WORK, jnp.minimum(i, chunks - 1)) // 32)
            share(slot).wait_recv()
            for n in range(cols // 256):
                part = pl.ds(n * 256, 256)
                gate = jnp.dot(xb[slot], wg[:, part], preferred_element_type=jnp.float32)
                up = jnp.dot(xb[slot], wu[:, part], preferred_element_type=jnp.float32)
                hid[:, part] = (jax.nn.silu(gate) * up).astype(hid.dtype)

        @pl.when(i >= 1)
        def _():
            for link in range(3):

                @pl.when(bit(arriving, link))
                def _():
                    fetch(slot_before, link).wait()
                    for n in range(wide // tile):
                        part = pl.ds(n * tile, tile)
                        acc[:, part] += got[link, :, part].astype(jnp.float32)

            give(i - 1).wait_recv()

            @pl.when(i - 1 >= STAGES)
            def _():
                sent(i - 1)

            for n in range(wide // tile):
                part = pl.ds(n * tile, tile)
                stage[lax.rem(i - 1, STAGES), :, part] = (
                    acc[:, part] + other[lax.rem(i - 1, 2), :, part].astype(jnp.float32)
                ).astype(stage.dtype)
            for link in range(3):

                @pl.when(leaving == 1 + link)
                def _():
                    sum_to(i - 1, slot_before, link).start()

            @pl.when(leaving == 0)
            def _():
                keep(i - 1, slot_before).start()

        @pl.when(i < chunks)
        def _():
            @pl.when(i >= 2)
            def _():
                give(i).wait_send()

            for n in range(wide // tile):
                part = pl.ds(n * tile, tile)
                both = jnp.dot(hid[...], wd[:, part], preferred_element_type=jnp.float32)
                acc[:, part] = both[:rows]
                term[lax.rem(i, 2), :, part] = both[rows:].astype(term.dtype)
            give(i).start()

    for i in range(2):
        give(i).wait_send()
    for i in range(STAGES):
        sent(i)

    @pl.loop(0, chunks)
    def _(j):
        code = pick(PASS, j)
        slot = slot_of(code // 8)
        for link in range(3):

            @pl.when(bit(lax.rem(code, 8), link))
            def _():
                rows_to(link, slot).wait_send()

        share(slot).wait_send()


def solution(mesh):
    def step(x, w_gate, w_up, w_down):
        total, depth = x.shape
        rows = total // PARTS
        chunks = 8 * PARTS
        cols = w_gate.shape[1]
        wide = w_down.shape[1]
        dma = pltpu.SemaphoreType.DMA
        b16, f32 = jnp.bfloat16, jnp.float32
        anywhere = pl.BlockSpec(memory_space=pl.ANY)
        out, _ = pl.pallas_call(
            kernel,
            name="ladder",
            out_shape=(
                jax.ShapeDtypeStruct((total, wide), b16),
                jax.ShapeDtypeStruct((chunks * 3, rows, wide), b16),
            ),
            in_specs=[anywhere] * 4,
            out_specs=(anywhere, anywhere),
            scratch_shapes=[
                pltpu.VMEM((depth, cols), b16),
                pltpu.VMEM((depth, cols), b16),
                pltpu.VMEM((cols, wide), b16),
                pltpu.VMEM((chunks, 2 * rows, depth), b16),
                pltpu.VMEM((rows, wide), f32),
                pltpu.VMEM((2 * rows, cols), b16),
                pltpu.VMEM((2, rows, wide), b16),
                pltpu.VMEM((2, rows, wide), b16),
                pltpu.VMEM((3, rows, wide), b16),
                pltpu.VMEM((STAGES, rows, wide), b16),
                dma((3,)), dma((PARTS,)), dma((3,)),
                dma((3, chunks)), dma((chunks,)), dma((chunks,)), dma((chunks,)),
                dma((2,)), dma((2,)), dma((STAGES,)), dma((chunks * 3,)),
            ],
            compiler_params=pltpu.CompilerParams(
                collective_id=0, has_side_effects=True, vmem_limit_bytes=67043328
            ),
            cost_estimate=pl.CostEstimate(
                flops=2 * 16 * total * depth * cols * 3,
                bytes_accessed=3 * depth * cols * 2 + 64 * total * depth * 2,
                transcendentals=16 * total * cols,
            ),
        )(x, w_gate, w_up, w_down)
        return out

    return jax.shard_map(
        step,
        mesh=mesh,
        in_specs=(P(("dp", "tp"), None), P(None, "tp"), P(None, "tp"), P("tp", None)),
        out_specs=P(("dp", "tp"), None),
        check_vma=False,
    )
```

```python
import functools

import jax
import jax.numpy as jnp
from jax import lax
from jax.experimental import pallas as pl
from jax.experimental.pallas import tpu as pltpu
from jax.sharding import PartitionSpec as P

PARTS = 4
STAGES = 8
MESH = pl.DeviceIdType.MESH
PASS = (
    (
        5, 28, 12, 21, 57, 41, 148, 49, 89, 132, 65, 220,
        81, 113, 120, 192, 240, 168, 104, 225, 184, 248, 96, 232,
        208, 200, 161, 72, 136, 32, 176, 152,
    ),
    (
        63, 37, 47, 55, 90, 67, 28, 20, 0, 13, 82, 123,
        115, 192, 132, 144, 180, 107, 227, 216, 240, 254, 234, 184,
        75, 202, 162, 138, 154, 96, 168, 208,
    ),
)
PASS_END = (
    (
        7, 11, 11, 13, 15, 16, 16, 20, 21, 22, 22, 24,
        24, 24, 25, 25, 25, 27, 28, 28, 29, 31, 31, 31,
        32, 32, 32, 32, 32, 32, 32, 32,
    ),
    (
        15, 16, 20, 21, 25, 25, 25, 25, 26, 27, 27, 27,
        27, 28, 31, 31, 31, 31, 31, 31, 31, 32, 32, 32,
        32, 32, 32, 32, 32, 32, 32, 32,
    ),
)
WORK = (
    (
        579, 161, 355, 867, 451, 481, 771, 963, 417, 897, 999, 321,
        679, 737, 935, 391, 259, 817, 641, 839, 513, 295, 705, 135,
        231, 625, 561, 199, 80, 100, 20, 36,
    ),
    (
        35, 587, 707, 899, 97, 875, 363, 481, 433, 802, 777, 985,
        641, 1007, 529, 753, 681, 943, 463, 395, 630, 562, 271, 857,
        82, 299, 22, 327, 156, 252, 180, 216,
    ),
)


def kernel(x_ref, wg_ref, wu_ref, wd_ref, out_ref, sum_ref,
           wg, wu, wd, xb, acc, hid, term, other, got, stage,
           w_sem, own_sem, load_sem,
           x_send, x_recv, d_send, d_recv, t_send, t_recv, s_send, s_recv):
    chunks = 8 * PARTS
    rows = xb.shape[1] // 2
    depth, cols = wg.shape
    wide = wd.shape[1]
    tile = 512

    dp = lax.axis_index("dp")
    tp = lax.axis_index("tp")
    core = lax.rem(tp, 2)
    chip = tp // 2
    y = chip // 4
    z = lax.rem(chip, 4)
    flip = z // 2
    outer = (z == 0) | (z == 3)
    away = 2 - 4 * flip
    mate = (dp, tp + 1 - 2 * core)
    peers = ((dp, tp + 8 - 16 * y), (dp, tp - away), (dp, tp + away))

    def pick(table, i):
        value = jnp.where(outer, table[0][0], table[1][0])
        for n in range(1, len(table[0])):
            value = jnp.where(i == n, jnp.where(outer, table[0][n], table[1][n]), value)
        return value

    def slot_of(chunk):
        source = chunk // PARTS
        sy = lax.rem(source // 4 + y, 2)
        sz = lax.rem(source, 4)
        sz = sz + flip * (3 - 2 * sz)
        return (sy * 4 + sz) * PARTS + lax.rem(chunk, PARTS)

    def bit(mask, n):
        return lax.rem(mask // (1 << n), 2) == 1

    loads = [
        pltpu.make_async_copy(src, dst, w_sem.at[n])
        for n, (src, dst) in enumerate(((wg_ref, wg), (wu_ref, wu), (wd_ref, wd)))
    ]
    mine = [
        pltpu.make_async_copy(
            x_ref.at[pl.ds(q * rows, rows)],
            xb.at[chip * PARTS + q, pl.ds(0, rows)],
            own_sem.at[q],
        )
        for q in range(PARTS)
    ]
    for copy in mine + loads:
        copy.start()

    barrier = pltpu.get_barrier_semaphore()
    for peer in (mate, peers[0], peers[2]):
        pl.semaphore_signal(barrier, inc=1, device_id=peer, device_id_type=MESH)

    @pl.when(jnp.logical_not(outer))
    def _():
        pl.semaphore_signal(barrier, inc=1, device_id=peers[1], device_id_type=MESH)

    pl.semaphore_wait(barrier, jnp.where(outer, 3, 4))

    def remote(src, dst, send, recv, peer):
        return pltpu.make_async_remote_copy(
            src_ref=src, dst_ref=dst, send_sem=send, recv_sem=recv,
            device_id=peer, device_id_type=MESH,
        )

    def rows_to(link, slot, src=None):
        here = xb.at[slot, pl.ds(0, rows)]
        return remote(
            here if src is None else src, here,
            x_send.at[link, slot], x_recv.at[slot], peers[link],
        )

    def share(slot, src=None):
        return remote(
            xb.at[slot, pl.ds(0, rows)] if src is None else src,
            xb.at[slot, pl.ds(rows, rows)],
            d_send.at[slot], d_recv.at[slot], mate,
        )

    def give(i):
        n = lax.rem(i, 2)
        return remote(term.at[n], other.at[n], t_send.at[n], t_recv.at[n], mate)

    def landing(slot, link):
        return sum_ref.at[slot * 3 + link]

    def fetch(slot, link):
        return pltpu.make_async_copy(landing(slot, link), got.at[link], load_sem.at[link])

    def sum_to(i, slot, link):
        n = lax.rem(i, STAGES)
        there = 0 if link == 0 else 2 if link == 1 else jnp.where(outer, 1, 2)
        return remote(
            stage.at[n], landing(slot, there), s_send.at[n], s_recv.at[slot * 3 + there],
            peers[link],
        )

    def keep(i, slot):
        n = lax.rem(i, STAGES)
        q = lax.rem(slot, PARTS)
        return pltpu.make_async_copy(
            stage.at[n], out_ref.at[pl.ds(pl.multiple_of(q * rows, rows), rows)], s_send.at[n]
        )

    def sent(i):
        n = lax.rem(i, STAGES)
        pltpu.make_async_copy(stage.at[n], stage.at[n], s_send.at[n]).wait()

    def pass_on(j, own=False):
        code = pick(PASS, j)
        chunk = code // 8
        mask = lax.rem(code, 8)
        slot = slot_of(chunk)
        src = None
        if own:
            q = lax.rem(chunk, PARTS)
            src = x_ref.at[pl.ds(pl.multiple_of(q * rows, rows), rows)]
        else:
            rows_to(0, slot).wait_recv()
        for link in (2, 1, 0):

            @pl.when(bit(mask, link))
            def _():
                rows_to(link, slot, src).start()

        share(slot, src).start()

    for j in range(PARTS):
        pass_on(j, own=True)
    for copy in mine + loads:
        copy.wait()

    @pl.loop(0, chunks + 1)
    def _(i):
        begin = jnp.where(i == 0, PARTS, pick(PASS_END, jnp.maximum(i - 1, 0)))
        end = pick(PASS_END, jnp.minimum(i, chunks - 1))

        def passing(j, carry):
            pass_on(j)
            return carry

        lax.fori_loop(begin, end, passing, 0)

        before = pick(WORK, jnp.maximum(i - 1, 0))
        slot_before = slot_of(before // 32)
        arriving = lax.rem(before // 4, 8)
        leaving = lax.rem(before, 4)

        @pl.when(i >= 1)
        def _():
            for link in range(3):

                @pl.when(bit(arriving, link))
                def _():
                    remote(
                        landing(slot_before, link), landing(slot_before, link),
                        s_send.at[0], s_recv.at[slot_before * 3 + link], mate,
                    ).wait_recv()
                    fetch(slot_before, link).start()

        @pl.when(i < chunks)
        def _():
            slot = slot_of(pick(WORK, jnp.minimum(i, chunks - 1)) // 32)
            share(slot).wait_recv()
            for n in range(cols // 256):
                part = pl.ds(n * 256, 256)
                gate = jnp.dot(xb[slot], wg[:, part], preferred_element_type=jnp.float32)
                up = jnp.dot(xb[slot], wu[:, part], preferred_element_type=jnp.float32)
                hid[:, part] = (jax.nn.silu(gate) * up).astype(hid.dtype)

        @pl.when(i >= 1)
        def _():
            for link in range(3):

                @pl.when(bit(arriving, link))
                def _():
                    fetch(slot_before, link).wait()
                    for n in range(wide // tile):
                        part = pl.ds(n * tile, tile)
                        acc[:, part] += got[link, :, part].astype(jnp.float32)

            give(i - 1).wait_recv()

            @pl.when(i - 1 >= STAGES)
            def _():
                sent(i - 1)

            for n in range(wide // tile):
                part = pl.ds(n * tile, tile)
                stage[lax.rem(i - 1, STAGES), :, part] = (
                    acc[:, part] + other[lax.rem(i - 1, 2), :, part].astype(jnp.float32)
                ).astype(stage.dtype)
            for link in range(3):

                @pl.when(leaving == 1 + link)
                def _():
                    sum_to(i - 1, slot_before, link).start()

            @pl.when(leaving == 0)
            def _():
                keep(i - 1, slot_before).start()

        @pl.when(i < chunks)
        def _():
            @pl.when(i >= 2)
            def _():
                give(i).wait_send()

            for n in range(wide // tile):
                part = pl.ds(n * tile, tile)
                both = jnp.dot(hid[...], wd[:, part], preferred_element_type=jnp.float32)
                acc[:, part] = both[:rows]
                term[lax.rem(i, 2), :, part] = both[rows:].astype(term.dtype)
            give(i).start()

    for i in range(2):
        give(i).wait_send()
    for i in range(STAGES):
        sent(i)

    @pl.loop(0, chunks)
    def _(j):
        code = pick(PASS, j)
        slot = slot_of(code // 8)
        for link in range(3):

            @pl.when(bit(lax.rem(code, 8), link))
            def _():
                rows_to(link, slot).wait_send()

        share(slot).wait_send()


def solution(mesh):
    def step(x, w_gate, w_up, w_down):
        total, depth = x.shape
        rows = total // PARTS
        chunks = 8 * PARTS
        cols = w_gate.shape[1]
        wide = w_down.shape[1]
        dma = pltpu.SemaphoreType.DMA
        b16, f32 = jnp.bfloat16, jnp.float32
        anywhere = pl.BlockSpec(memory_space=pl.ANY)
        out, _ = pl.pallas_call(
            kernel,
            name="ladder",
            out_shape=(
                jax.ShapeDtypeStruct((total, wide), b16),
                jax.ShapeDtypeStruct((chunks * 3, rows, wide), b16),
            ),
            in_specs=[anywhere] * 4,
            out_specs=(anywhere, anywhere),
            scratch_shapes=[
                pltpu.VMEM((depth, cols), b16),
                pltpu.VMEM((depth, cols), b16),
                pltpu.VMEM((cols, wide), b16),
                pltpu.VMEM((chunks, 2 * rows, depth), b16),
                pltpu.VMEM((rows, wide), f32),
                pltpu.VMEM((2 * rows, cols), b16),
                pltpu.VMEM((2, rows, wide), b16),
                pltpu.VMEM((2, rows, wide), b16),
                pltpu.VMEM((3, rows, wide), b16),
                pltpu.VMEM((STAGES, rows, wide), b16),
                dma((3,)), dma((PARTS,)), dma((3,)),
                dma((3, chunks)), dma((chunks,)), dma((chunks,)), dma((chunks,)),
                dma((2,)), dma((2,)), dma((STAGES,)), dma((chunks * 3,)),
            ],
            compiler_params=pltpu.CompilerParams(
                collective_id=0, has_side_effects=True, vmem_limit_bytes=67043328
            ),
            cost_estimate=pl.CostEstimate(
                flops=2 * 16 * total * depth * cols * 3,
                bytes_accessed=3 * depth * cols * 2 + 64 * total * depth * 2,
                transcendentals=16 * total * cols,
            ),
        )(x, w_gate, w_up, w_down)
        return out

    return jax.shard_map(
        step,
        mesh=mesh,
        in_specs=(P(("dp", "tp"), None), P(None, "tp"), P(None, "tp"), P("tp", None)),
        out_specs=P(("dp", "tp"), None),
        check_vma=False,
    )
```

```python
import functools

import jax
import jax.numpy as jnp
from jax import lax
from jax.experimental import pallas as pl
from jax.experimental.pallas import tpu as pltpu
from jax.sharding import PartitionSpec as P

PARTS = 4
STAGES = 16
MESH = pl.DeviceIdType.MESH
PASS = (
    (
        53, 28, 37, 61, 1, 21, 9, 45, 292, 260, 105, 268,
        65, 276, 329, 300, 97, 364, 81, 249, 320, 72, 352, 241,
        176, 336, 153, 504, 217, 496, 408, 209, 185, 489, 481, 401,
        112, 472, 432, 464, 304, 448, 376, 424, 440, 456, 392, 192,
        232, 224, 384, 416, 200, 128, 144, 136, 368, 312, 120, 168,
        160, 345, 280, 88,
    ),
    (
        127, 92, 77, 87, 119, 106, 99, 67, 61, 334, 155, 53,
        29, 292, 179, 340, 250, 20, 243, 378, 261, 324, 187, 219,
        32, 300, 434, 144, 210, 316, 364, 356, 269, 44, 490, 483,
        402, 451, 394, 504, 387, 412, 427, 459, 276, 224, 419, 194,
        496, 440, 130, 8, 202, 232, 138, 370, 170, 464, 304, 162,
        472, 346, 282, 0,
    ),
)
PASS_END = (
    (
        18, 22, 26, 27, 28, 33, 33, 35, 38, 39, 43, 43,
        46, 49, 52, 53, 53, 57, 57, 58, 58, 61, 62, 62,
        63, 63, 63, 64, 64, 64, 64, 64,
    ),
    (
        23, 33, 34, 40, 42, 50, 50, 52, 52, 52, 52, 60,
        62, 62, 63, 63, 63, 63, 63, 63, 63, 64, 64, 64,
        64, 64, 64, 64, 64, 64, 64, 64,
    ),
)
WORK = (
    (
        6243, 20579, 15395, 22627, 18465, 13347, 11363, 30753, 31971, 4195, 29923, 25697,
        28705, 27747, 24609, 14567, 26657, 12519, 8423, 23585, 16417, 10471, 9319, 21537,
        7399, 17969, 20017, 5351, 2708, 1156, 660, 3732,
    ),
    (
        1121, 16483, 15401, 30755, 13865, 24611, 11563, 29233, 32239, 18481, 22825, 3138,
        26657, 30191, 20793, 25891, 28139, 18006, 14827, 20050, 12783, 24113, 21553, 8683,
        2774, 10735, 594, 9707, 5020, 7580, 7068, 6044,
    ),
)


def kernel(x_ref, wg_ref, wu_ref, wd_ref, out_ref, sum_ref,
           wg, wu, wd, xb, acc, hid, term, other, got, stage,
           w_sem, own_sem, load_sem,
           x_send, x_recv, d_send, d_recv, t_send, t_recv, s_send, s_recv):
    chunks = 8 * PARTS
    rows = xb.shape[1] // 2
    half = rows // 2
    depth, cols = wg.shape
    wide = wd.shape[1]
    tile = 512

    dp = lax.axis_index("dp")
    tp = lax.axis_index("tp")
    core = lax.rem(tp, 2)
    chip = tp // 2
    y = chip // 4
    z = lax.rem(chip, 4)
    flip = z // 2
    outer = (z == 0) | (z == 3)
    away = 2 - 4 * flip
    mate = (dp, tp + 1 - 2 * core)
    peers = ((dp, tp + 8 - 16 * y), (dp, tp - away), (dp, tp + away))

    def pick(table, i):
        value = jnp.where(outer, table[0][0], table[1][0])
        for n in range(1, len(table[0])):
            value = jnp.where(i == n, jnp.where(outer, table[0][n], table[1][n]), value)
        return value

    def slot_of(chunk):
        source = chunk // PARTS
        sy = lax.rem(source // 4 + y, 2)
        sz = lax.rem(source, 4)
        sz = sz + flip * (3 - 2 * sz)
        return (sy * 4 + sz) * PARTS + lax.rem(chunk, PARTS)

    def bit(mask, n):
        return lax.rem(mask // (1 << n), 2) == 1

    loads = [
        pltpu.make_async_copy(src, dst, w_sem.at[n])
        for n, (src, dst) in enumerate(((wg_ref, wg), (wu_ref, wu), (wd_ref, wd)))
    ]
    mine = [
        pltpu.make_async_copy(
            x_ref.at[pl.ds(q * rows, rows)],
            xb.at[chip * PARTS + q, pl.ds(0, rows)],
            own_sem.at[q],
        )
        for q in range(PARTS)
    ]
    for copy in mine + loads:
        copy.start()

    barrier = pltpu.get_barrier_semaphore()
    for peer in (mate, peers[0], peers[2]):
        pl.semaphore_signal(barrier, inc=1, device_id=peer, device_id_type=MESH)

    @pl.when(jnp.logical_not(outer))
    def _():
        pl.semaphore_signal(barrier, inc=1, device_id=peers[1], device_id_type=MESH)

    pl.semaphore_wait(barrier, jnp.where(outer, 3, 4))

    def remote(src, dst, send, recv, peer):
        return pltpu.make_async_remote_copy(
            src_ref=src, dst_ref=dst, send_sem=send, recv_sem=recv,
            device_id=peer, device_id_type=MESH,
        )

    def piece_at(core_rows, piece):
        start = core_rows * rows + lax.rem(piece, 2) * half
        return xb.at[piece // 2, pl.ds(pl.multiple_of(start, half), half)]

    def rows_to(link, piece, j=0, src=None):
        here = piece_at(0, piece)
        return remote(
            here if src is None else src, here,
            x_send.at[link, j], x_recv.at[piece], peers[link],
        )

    def share(piece, j=0, src=None):
        return remote(
            piece_at(0, piece) if src is None else src, piece_at(1, piece),
            d_send.at[j], d_recv.at[piece], mate,
        )

    def give(i):
        n = lax.rem(i, 2)
        return remote(term.at[n], other.at[n], t_send.at[n], t_recv.at[n], mate)

    def landing(piece, link):
        return sum_ref.at[piece * 3 + link]

    def fetch(piece, h, link):
        return pltpu.make_async_copy(
            landing(piece, link), got.at[link, pl.ds(h * half, half)], load_sem.at[link, h]
        )

    def staged(i, h):
        return stage.at[lax.rem(i, STAGES), pl.ds(h * half, half)]

    def sum_to(i, h, piece, link):
        there = 0 if link == 0 else 2 if link == 1 else jnp.where(outer, 1, 2)
        return remote(
            staged(i, h), landing(piece, there), s_send.at[lax.rem(i, STAGES), h],
            s_recv.at[piece * 3 + there], peers[link],
        )

    def keep(i, h, piece):
        start = lax.rem(piece, 2 * PARTS) * half
        return pltpu.make_async_copy(
            staged(i, h), out_ref.at[pl.ds(pl.multiple_of(start, half), half)],
            s_send.at[lax.rem(i, STAGES), h],
        )

    def sent(i):
        for h in range(2):
            pltpu.make_async_copy(
                staged(i, h), staged(i, h), s_send.at[lax.rem(i, STAGES), h]
            ).wait()

    def piece_of(code):
        name = code // 8
        return slot_of(name // 2) * 2 + lax.rem(name, 2)

    def pass_on(j, own=False):
        code = pick(PASS, j)
        mask = lax.rem(code, 8)
        piece = piece_of(code)
        src = None
        if own:
            start = lax.rem(piece, 2 * PARTS) * half
            src = x_ref.at[pl.ds(pl.multiple_of(start, half), half)]
        else:
            rows_to(0, piece).wait_recv()
        for link in (2, 1, 0):

            @pl.when(bit(mask, link))
            def _():
                rows_to(link, piece, j, src).start()

        share(piece, j, src).start()

    for j in range(2 * PARTS):
        pass_on(j, own=True)
    for copy in mine + loads:
        copy.wait()

    @pl.loop(0, chunks + 1)
    def _(i):
        begin = jnp.where(i == 0, 2 * PARTS, pick(PASS_END, jnp.maximum(i - 1, 0)))
        end = pick(PASS_END, jnp.minimum(i, chunks - 1))

        def passing(j, carry):
            pass_on(j)
            return carry

        lax.fori_loop(begin, end, passing, 0)

        before = pick(WORK, jnp.maximum(i - 1, 0))
        slot_before = slot_of(before // 1024)
        halves = (lax.rem(before, 32), lax.rem(before // 32, 32))

        @pl.when(i >= 1)
        def _():
            for h in range(2):
                piece = slot_before * 2 + h
                for link in range(3):

                    @pl.when(bit(halves[h] // 4, link))
                    def _():
                        remote(
                            landing(piece, link), landing(piece, link),
                            s_send.at[0, 0], s_recv.at[piece * 3 + link], mate,
                        ).wait_recv()
                        fetch(piece, h, link).start()

        @pl.when(i < chunks)
        def _():
            slot = slot_of(pick(WORK, jnp.minimum(i, chunks - 1)) // 1024)
            for h in range(2):
                share(slot * 2 + h).wait_recv()
            for n in range(cols // 256):
                part = pl.ds(n * 256, 256)
                gate = jnp.dot(xb[slot], wg[:, part], preferred_element_type=jnp.float32)
                up = jnp.dot(xb[slot], wu[:, part], preferred_element_type=jnp.float32)
                hid[:, part] = (jax.nn.silu(gate) * up).astype(hid.dtype)

        @pl.when(i >= 1)
        def _():
            for h in range(2):
                for link in range(3):

                    @pl.when(bit(halves[h] // 4, link))
                    def _():
                        fetch(slot_before * 2 + h, h, link).wait()
                        for n in range(wide // tile):
                            at = (pl.ds(h * half, half), pl.ds(n * tile, tile))
                            acc[at] += got[(link, *at)].astype(jnp.float32)

            give(i - 1).wait_recv()

            @pl.when(i - 1 >= STAGES)
            def _():
                sent(i - 1)

            for n in range(wide // tile):
                part = pl.ds(n * tile, tile)
                stage[lax.rem(i - 1, STAGES), :, part] = (
                    acc[:, part] + other[lax.rem(i - 1, 2), :, part].astype(jnp.float32)
                ).astype(stage.dtype)
            for h in range(2):
                piece = slot_before * 2 + h
                leaving = lax.rem(halves[h], 4)
                for link in range(3):

                    @pl.when(leaving == 1 + link)
                    def _():
                        sum_to(i - 1, h, piece, link).start()

                @pl.when(leaving == 0)
                def _():
                    keep(i - 1, h, piece).start()

        @pl.when(i < chunks)
        def _():
            @pl.when(i >= 2)
            def _():
                give(i).wait_send()

            for n in range(wide // tile):
                part = pl.ds(n * tile, tile)
                both = jnp.dot(hid[...], wd[:, part], preferred_element_type=jnp.float32)
                acc[:, part] = both[:rows]
                term[lax.rem(i, 2), :, part] = both[rows:].astype(term.dtype)
            give(i).start()

    for i in range(2):
        give(i).wait_send()
    for i in range(STAGES):
        sent(i)

    for kind, here in enumerate((outer, jnp.logical_not(outer))):

        @pl.when(here)
        def _():
            for j, code in enumerate(PASS[kind]):
                for link in range(3):
                    if code >> link & 1:
                        rows_to(link, 0, j).wait_send()
                share(0, j).wait_send()


def solution(mesh):
    def step(x, w_gate, w_up, w_down):
        total, depth = x.shape
        rows = total // PARTS
        chunks = 8 * PARTS
        cols = w_gate.shape[1]
        wide = w_down.shape[1]
        dma = pltpu.SemaphoreType.DMA
        b16, f32 = jnp.bfloat16, jnp.float32
        anywhere = pl.BlockSpec(memory_space=pl.ANY)
        out, _ = pl.pallas_call(
            kernel,
            name="ladder",
            out_shape=(
                jax.ShapeDtypeStruct((total, wide), b16),
                jax.ShapeDtypeStruct((chunks * 6, rows // 2, wide), b16),
            ),
            in_specs=[anywhere] * 4,
            out_specs=(anywhere, anywhere),
            scratch_shapes=[
                pltpu.VMEM((depth, cols), b16),
                pltpu.VMEM((depth, cols), b16),
                pltpu.VMEM((cols, wide), b16),
                pltpu.VMEM((chunks, 2 * rows, depth), b16),
                pltpu.VMEM((rows, wide), f32),
                pltpu.VMEM((2 * rows, cols), b16),
                pltpu.VMEM((2, rows, wide), b16),
                pltpu.VMEM((2, rows, wide), b16),
                pltpu.VMEM((3, rows, wide), b16),
                pltpu.VMEM((STAGES, rows, wide), b16),
                dma((3,)), dma((PARTS,)), dma((3, 2)),
                dma((3, 2 * chunks)), dma((2 * chunks,)), dma((2 * chunks,)), dma((2 * chunks,)),
                dma((2,)), dma((2,)), dma((STAGES, 2)), dma((chunks * 6,)),
            ],
            compiler_params=pltpu.CompilerParams(
                collective_id=0, has_side_effects=True, vmem_limit_bytes=67043328
            ),
            cost_estimate=pl.CostEstimate(
                flops=2 * 16 * total * depth * cols * 3,
                bytes_accessed=3 * depth * cols * 2 + 64 * total * depth * 2,
                transcendentals=16 * total * cols,
            ),
        )(x, w_gate, w_up, w_down)
        return out

    return jax.shard_map(
        step,
        mesh=mesh,
        in_specs=(P(("dp", "tp"), None), P(None, "tp"), P(None, "tp"), P("tp", None)),
        out_specs=P(("dp", "tp"), None),
        check_vma=False,
    )
```
